8 devices in a mesh: req: 2 (over z, y), dap: 4 (over x, core).
Axes of the slice: x: 2, y: 2, z: 1, core: 2. Of those that a mesh axis runs over, the one named last changes fastest.
Arguments:
- msa_act: bfloat16 [512, 256, 256], P(('req', 'dap')), parts along dimension 0
- pair_act: bfloat16 [512, 256, 128], P(('req', 'dap')), parts along dimension 0
- msa_mask: int32 [512, 256], P(('req', 'dap')), parts along dimension 0
- pair_mask: int32 [512, 256], P(('req', 'dap')), parts along dimension 0
- row_qkvg: bfloat16 [2, 256, 1024], replicated
- row_bias: bfloat16 [2, 128, 8], replicated
- row_out: bfloat16 [2, 256, 256], replicated
- col_qkvg: bfloat16 [2, 256, 1024], replicated
- col_out: bfloat16 [2, 256, 256], replicated
- mtr_in: bfloat16 [2, 256, 1024], replicated
- mtr_out: bfloat16 [2, 1024, 256], replicated
- opm_proj: bfloat16 [2, 256, 64], replicated
- opm_out: bfloat16 [2, 1024, 128], replicated
- tmo_proj: bfloat16 [2, 128, 640], replicated
- tmo_out: bfloat16 [2, 128, 128], replicated
- tmi_proj: bfloat16 [2, 128, 640], replicated
- tmi_out: bfloat16 [2, 128, 128], replicated
- tas_qkvg: bfloat16 [2, 128, 512], replicated
- tas_bias: bfloat16 [2, 128, 4], replicated
- tas_out: bfloat16 [2, 128, 128], replicated
- tae_qkvg: bfloat16 [2, 128, 512], replicated
- tae_bias: bfloat16 [2, 128, 4], replicated
- tae_out: bfloat16 [2, 128, 128], replicated
- ptr_in: bfloat16 [2, 128, 512], replicated
- ptr_out: bfloat16 [2, 512, 128], replicated
Outputs:
- output 1: bfloat16 [512, 256, 256], P(('req', 'dap')), parts along dimension 0
- output 2: bfloat16 [512, 256, 128], P(('req', 'dap')), parts along dimension 0
There are 2 independent parts. The reference program is written for one: setup_inputs(seed, part) draws one part's arguments, and reference() takes and returns one part's arrays. A program takes and returns all parts, laid end to end along the dimension named above; an argument that names none is the same for every part.
All inputs are finite; a program needn't handle non-finite values.
Results may differ from the reference program's by a relative error of at most 0.02.
Values are sent between devices in bfloat16 or wider.
A program may use at most 1 GiB of HBM per device.

```python
import jax
import jax.numpy as jnp
from jax import lax

SEQ = 256
RES = 256
MSA_DIM = 256
PAIR_DIM = 128
MSA_HEADS = 8
MSA_HEAD_DIM = 32
PAIR_HEADS = 4
PAIR_HEAD_DIM = 32
OPM_DIM = 32
TRI_DIM = 128
LAYERS = 2

WEIGHT_NAMES = ('row_qkvg', 'row_bias', 'row_out', 'col_qkvg', 'col_out', 'mtr_in', 'mtr_out', 'opm_proj', 'opm_out', 'tmo_proj', 'tmo_out', 'tmi_proj', 'tmi_out', 'tas_qkvg', 'tas_bias', 'tas_out', 'tae_qkvg', 'tae_bias', 'tae_out', 'ptr_in', 'ptr_out')


def weight_fans():
    msa_width = MSA_HEADS * MSA_HEAD_DIM
    pair_width = PAIR_HEADS * PAIR_HEAD_DIM
    return ((MSA_DIM, 4 * msa_width), (PAIR_DIM, MSA_HEADS), (msa_width, MSA_DIM),
            (MSA_DIM, 4 * msa_width), (msa_width, MSA_DIM),
            (MSA_DIM, 4 * MSA_DIM), (4 * MSA_DIM, MSA_DIM),
            (MSA_DIM, 2 * OPM_DIM), (OPM_DIM * OPM_DIM, PAIR_DIM),
            (PAIR_DIM, 4 * TRI_DIM + PAIR_DIM), (TRI_DIM, PAIR_DIM),
            (PAIR_DIM, 4 * TRI_DIM + PAIR_DIM), (TRI_DIM, PAIR_DIM),
            (PAIR_DIM, 4 * pair_width), (PAIR_DIM, PAIR_HEADS), (pair_width, PAIR_DIM),
            (PAIR_DIM, 4 * pair_width), (PAIR_DIM, PAIR_HEADS), (pair_width, PAIR_DIM),
            (PAIR_DIM, 4 * PAIR_DIM), (4 * PAIR_DIM, PAIR_DIM))


def draw_masks(mask_key):
    key_list = jax.random.split(mask_key, 4)
    pad_len = jax.random.randint(key_list[0], (), 1, RES // 16 + 1)
    res_ids = jnp.arange(RES)
    seq_ids = jnp.arange(SEQ)[:, None]
    is_valid = res_ids < RES - pad_len
    shallow = jax.random.randint(key_list[1], (RES,), 0, 4) == 0
    depths = jnp.where(shallow, jax.random.randint(key_list[2], (RES,), 1, SEQ // 4 + 1), SEQ)
    kept_mask = (jax.random.randint(key_list[3], (SEQ, RES), 0, 8) != 0) | (seq_ids == 0)
    msa_mask = ((seq_ids < depths[None, :]) & kept_mask & is_valid[None, :]).astype(jnp.int32)
    pair_mask = (is_valid[:, None] & is_valid[None, :]).astype(jnp.int32)
    return msa_mask, pair_mask


def setup_inputs(seed: int = 0, part: int = 0) -> dict:
    part_key = jax.random.fold_in(jax.random.key(seed), part)
    key_list = jax.random.split(part_key, 3)
    shared = jax.random.normal(key_list[0], (1, RES, MSA_DIM), jnp.float32)
    spread = jax.random.normal(key_list[1], (SEQ, RES, MSA_DIM), jnp.float32)
    msa_act = (shared + spread).astype(jnp.bfloat16)
    pair_act = jax.random.normal(key_list[2], (RES, RES, PAIR_DIM), jnp.float32).astype(jnp.bfloat16)
    msa_mask, pair_mask = draw_masks(jax.random.fold_in(part_key, 5))
    inputs = {'msa_act': msa_act, 'pair_act': pair_act, 'msa_mask': msa_mask, 'pair_mask': pair_mask}
    weight_key = jax.random.key(seed + 1)
    for w_index, fan_pair in enumerate(weight_fans()):
        sample = jax.random.normal(jax.random.fold_in(weight_key, w_index), (LAYERS,) + fan_pair, jnp.float32)
        inputs[WEIGHT_NAMES[w_index]] = (sample * fan_pair[0] ** -0.5).astype(jnp.bfloat16)
    return inputs


def layer_norm(x):
    values = x.astype(jnp.float32)
    centered = values - jnp.mean(values, axis=-1, keepdims=True)
    variance = jnp.mean(centered * centered, axis=-1, keepdims=True)
    return (centered * lax.rsqrt(variance + 1e-5)).astype(jnp.bfloat16)


def linear(x, weight):
    flat_x = x.reshape(-1, x.shape[-1])
    result = jnp.dot(flat_x, weight, preferred_element_type=jnp.float32)
    return result.reshape(x.shape[:-1] + (weight.shape[-1],))


def residual(x, update):
    return (x.astype(jnp.float32) + update).astype(jnp.bfloat16)


def attend_row(x_row, bias_hij, mask_row, w_qkvg, w_out, num_heads):
    length = x_row.shape[0]
    head_width = w_out.shape[0]
    head_dim = head_width // num_heads
    projected = jnp.dot(x_row, w_qkvg, preferred_element_type=jnp.float32).astype(jnp.bfloat16).astype(jnp.float32)
    queries = projected[:, :head_width].reshape(length, num_heads, head_dim)
    keyset = projected[:, head_width:2 * head_width].reshape(length, num_heads, head_dim)
    valset = projected[:, 2 * head_width:3 * head_width].reshape(length, num_heads, head_dim)
    gate_act = jax.nn.sigmoid(projected[:, 3 * head_width:])
    logits = jnp.einsum('ihd,jhd->hij', queries, keyset) * head_dim ** -0.5 + bias_hij.astype(jnp.float32)
    logits = jnp.where(mask_row[None, None, :] > 0, logits, -1e9)
    attn_prob = jax.nn.softmax(logits, axis=-1).astype(jnp.bfloat16).astype(jnp.float32)
    attended = jnp.einsum('hij,jhd->ihd', attn_prob, valset).reshape(length, head_width)
    gated = (attended * gate_act).astype(jnp.bfloat16)
    return jnp.dot(gated, w_out, preferred_element_type=jnp.float32)


def row_attention(msa_act, pair_act, msa_mask, w_qkvg, w_bias, w_out):
    pair_bias = jnp.transpose(linear(layer_norm(pair_act), w_bias).astype(jnp.bfloat16), (2, 0, 1))
    msa_norm = layer_norm(msa_act)
    return lax.map(lambda item: attend_row(item[0], pair_bias, item[1], w_qkvg, w_out, w_bias.shape[1]), (msa_norm, msa_mask))


def column_attention(msa_act, msa_mask, w_qkvg, w_out, num_heads):
    msa_norm = jnp.swapaxes(layer_norm(msa_act), 0, 1)
    zero_bias = jnp.zeros((1, 1, 1), jnp.float32)
    update = lax.map(lambda item: attend_row(item[0], zero_bias, item[1], w_qkvg, w_out, num_heads), (msa_norm, msa_mask.T))
    return jnp.swapaxes(update, 0, 1)


def transition(x, w_in, w_out):
    hidden = jnp.maximum(linear(layer_norm(x), w_in), 0.0).astype(jnp.bfloat16)
    return linear(hidden, w_out)


def outer_product_mean(msa_act, msa_mask, w_proj, w_out):
    opm_dim = w_proj.shape[1] // 2
    projected = linear(layer_norm(msa_act), w_proj).astype(jnp.bfloat16)
    mask_bf = msa_mask.astype(jnp.bfloat16)[:, :, None]
    left_act = (projected[..., :opm_dim] * mask_bf).astype(jnp.float32)
    right_act = (projected[..., opm_dim:] * mask_bf).astype(jnp.float32)
    mask_f = msa_mask.astype(jnp.float32)
    overlap = jnp.dot(mask_f.T, mask_f)

    def outer_row(left_row):
        outer_prod = jnp.einsum('sc,sje->jce', left_row, right_act).astype(jnp.bfloat16)
        return linear(outer_prod.reshape(outer_prod.shape[0], opm_dim * opm_dim), w_out)

    update = lax.map(outer_row, jnp.swapaxes(left_act, 0, 1))
    return update / (1e-3 + overlap)[:, :, None]


def tri_mul(pair_act, pair_mask, w_proj, w_out, form):
    tri_dim = (w_proj.shape[1] - pair_act.shape[-1]) // 4
    projected = linear(layer_norm(pair_act), w_proj)
    mask_f = pair_mask.astype(jnp.float32)[:, :, None]
    left_act = (mask_f * jax.nn.sigmoid(projected[..., 2 * tri_dim:3 * tri_dim]) * projected[..., :tri_dim]).astype(jnp.bfloat16)
    right_act = (mask_f * jax.nn.sigmoid(projected[..., 3 * tri_dim:4 * tri_dim]) * projected[..., tri_dim:2 * tri_dim]).astype(jnp.bfloat16)
    gate_act = jax.nn.sigmoid(projected[..., 4 * tri_dim:])
    product = jnp.einsum(form, left_act.astype(jnp.float32), right_act.astype(jnp.float32))
    return gate_act * linear(layer_norm(product), w_out)


def tri_attention(pair_act, pair_mask, w_qkvg, w_bias, w_out):
    pair_norm = layer_norm(pair_act)
    pair_bias = jnp.transpose(linear(pair_norm, w_bias).astype(jnp.bfloat16), (2, 0, 1))
    return lax.map(lambda item: attend_row(item[0], pair_bias, item[1], w_qkvg, w_out, w_bias.shape[1]), (pair_norm, pair_mask))


def evoformer_block(msa_act, pair_act, msa_mask, pair_mask, layer_w):
    (row_qkvg, row_bias, row_out, col_qkvg, col_out, mtr_in, mtr_out, opm_proj, opm_out,
     tmo_proj, tmo_out, tmi_proj, tmi_out, tas_qkvg, tas_bias, tas_out,
     tae_qkvg, tae_bias, tae_out, ptr_in, ptr_out) = layer_w
    msa_act = residual(msa_act, row_attention(msa_act, pair_act, msa_mask, row_qkvg, row_bias, row_out))
    msa_act = residual(msa_act, column_attention(msa_act, msa_mask, col_qkvg, col_out, row_bias.shape[1]))
    msa_act = residual(msa_act, transition(msa_act, mtr_in, mtr_out))
    pair_act = residual(pair_act, outer_product_mean(msa_act, msa_mask, opm_proj, opm_out))
    pair_act = residual(pair_act, tri_mul(pair_act, pair_mask, tmo_proj, tmo_out, 'ikc,jkc->ijc'))
    pair_act = residual(pair_act, tri_mul(pair_act, pair_mask, tmi_proj, tmi_out, 'kic,kjc->ijc'))
    pair_act = residual(pair_act, tri_attention(pair_act, pair_mask, tas_qkvg, tas_bias, tas_out))
    pair_swap = jnp.swapaxes(pair_act, 0, 1)
    pair_act = residual(pair_act, jnp.swapaxes(tri_attention(pair_swap, pair_mask.T, tae_qkvg, tae_bias, tae_out), 0, 1))
    pair_act = residual(pair_act, transition(pair_act, ptr_in, ptr_out))
    return msa_act, pair_act


def reference(msa_act, pair_act, msa_mask, pair_mask, row_qkvg, row_bias, row_out, col_qkvg, col_out, mtr_in, mtr_out, opm_proj, opm_out, tmo_proj, tmo_out, tmi_proj, tmi_out, tas_qkvg, tas_bias, tas_out, tae_qkvg, tae_bias, tae_out, ptr_in, ptr_out):
    stacked = (row_qkvg, row_bias, row_out, col_qkvg, col_out, mtr_in, mtr_out, opm_proj, opm_out,
               tmo_proj, tmo_out, tmi_proj, tmi_out, tas_qkvg, tas_bias, tas_out,
               tae_qkvg, tae_bias, tae_out, ptr_in, ptr_out)

    def step(carry, layer_w):
        return evoformer_block(carry[0], carry[1], msa_mask, pair_mask, layer_w), None

    carried, ignored = lax.scan(step, (msa_act, pair_act), stacked)
    return carried[0], carried[1]
```

```python
import functools

import jax
import jax.numpy as jnp
from jax import lax
from jax.experimental import pallas as pl
from jax.experimental.pallas import tpu as pltpu
from jax.sharding import PartitionSpec as P

GROUP_AXIS = 'dap'
PARTS_AXIS = 'req'
MASKED_LOGIT = -1e9


def layer_norm(x):
    values = x.astype(jnp.float32)
    centered = values - jnp.mean(values, axis=-1, keepdims=True)
    variance = jnp.mean(centered * centered, axis=-1, keepdims=True)
    return (centered * lax.rsqrt(variance + 1e-5)).astype(jnp.bfloat16)


def residual(x, update):
    return (x.astype(jnp.float32) + update).astype(jnp.bfloat16)


def dense(x, weight):
    return jnp.einsum('...c,cf->...f', x, weight, preferred_element_type=jnp.float32)


LOG2E = 1.4426950408889634
HEAD_DIM = 32


def norm_rows(values):
    centered = values - jnp.mean(values, axis=-1, keepdims=True)
    variance = jnp.mean(centered * centered, axis=-1, keepdims=True)
    return (centered * lax.rsqrt(variance + 1e-5)).astype(jnp.bfloat16)


def mm(a, b):
    return jnp.dot(a, b, preferred_element_type=jnp.float32)


def attn_kernel(*refs, has_bias, has_transition):
    refs = list(refs)
    x_ref, mask_ref = refs[:2]
    refs = refs[2:]
    bias_ref = refs.pop(0) if has_bias else None
    w_ref, wo_ref = refs[:2]
    out_ref = refs[-1]
    width = wo_ref.shape[0]
    x = x_ref[0].astype(jnp.float32)
    proj = mm(norm_rows(x), w_ref[...]).astype(jnp.bfloat16)
    q, k, v = proj[:, :width], proj[:, width:2 * width], proj[:, 2 * width:3 * width]
    gate = jax.nn.sigmoid(proj[:, 3 * width:].astype(jnp.float32))
    kept = mask_ref[0] > 0
    lane_head = lax.broadcasted_iota(jnp.int32, (1, width), 1) // HEAD_DIM
    attended = None
    for h in range(width // HEAD_DIM):
        pick = jnp.where(lane_head == h, 1.0, 0.0).astype(jnp.bfloat16)
        logits = lax.dot_general(q * pick, k, (((1,), (1,)), ((), ())), preferred_element_type=jnp.float32)
        logits = logits * (HEAD_DIM ** -0.5 * LOG2E)
        if has_bias:
            logits = logits + bias_ref[h]
        logits = jnp.where(kept, logits, -1e9 * LOG2E)
        weight = jnp.exp2(logits - jnp.max(logits, axis=-1, keepdims=True))
        prob = (weight * (1.0 / jnp.sum(weight, axis=-1, keepdims=True))).astype(jnp.bfloat16)
        part = mm(prob, v * pick)
        attended = part if attended is None else attended + part
    gated = (attended * gate).astype(jnp.bfloat16)
    y = (x + mm(gated, wo_ref[...])).astype(jnp.bfloat16)
    if has_transition:
        y32 = y.astype(jnp.float32)
        hidden = jnp.maximum(mm(norm_rows(y32), refs[2][...]), 0.0).astype(jnp.bfloat16)
        y = (y32 + mm(hidden, refs[3][...])).astype(jnp.bfloat16)
    out_ref[0] = y


def attention(x, mask, w_qkvg, w_out, pair_bias=None, w_trans=None):
    n, length, width = x.shape
    args = [x, mask.astype(jnp.float32)[:, None, :]]
    specs = [pl.BlockSpec((1, length, width), lambda i: (i, 0, 0)), pl.BlockSpec((1, 1, length), lambda i: (i, 0, 0))]

    def whole(a):
        args.append(a)
        specs.append(pl.BlockSpec(a.shape, lambda i: (0,) * a.ndim))

    if pair_bias is not None:
        whole(pair_bias.astype(jnp.float32) * LOG2E)
    whole(w_qkvg)
    whole(w_out)
    for w in w_trans or ():
        whole(w)
    heads = w_out.shape[0] // HEAD_DIM
    flops = 2 * n * length * (width * w_qkvg.shape[1] + 2 * length * w_out.shape[0] + w_out.size)
    return pl.pallas_call(
        functools.partial(attn_kernel, has_bias=pair_bias is not None, has_transition=w_trans is not None),
        grid=(n,), in_specs=specs, out_specs=specs[0],
        out_shape=jax.ShapeDtypeStruct(x.shape, x.dtype),
        compiler_params=pltpu.CompilerParams(dimension_semantics=("arbitrary",), vmem_limit_bytes=48 << 20),
        cost_estimate=pl.CostEstimate(flops=flops, bytes_accessed=4 * x.size, transcendentals=n * heads * length * length),
    )(*args)


def pair_bias_full(pair_rows, w_bias):
    return lax.all_gather(head_bias(layer_norm(pair_rows), w_bias), GROUP_AXIS, axis=1, tiled=True)


def head_bias(pair_norm, w_bias):
    return jnp.einsum('ijc,ch->hij', pair_norm, w_bias, preferred_element_type=jnp.float32).astype(jnp.bfloat16)


def outer_update(array_b7, res_mask, full_mask, w_proj, w_out):
    opm_dim = w_proj.shape[1] // 2
    projected = dense(layer_norm(array_b7), w_proj).astype(jnp.bfloat16)
    mask_bf = res_mask.T.astype(jnp.bfloat16)[:, :, None]
    left_act = projected[..., :opm_dim] * mask_bf
    right_act = projected[..., opm_dim:] * mask_bf
    right_full = lax.all_gather(right_act, GROUP_AXIS, axis=0, tiled=True)
    outer_prod = jnp.einsum('isc,jse->ijce', left_act, right_full, preferred_element_type=jnp.float32).astype(jnp.bfloat16)
    n_rows, n_cols = outer_prod.shape[:2]
    update = dense(outer_prod.reshape(n_rows, n_cols, opm_dim * opm_dim), w_out)
    overlap = jnp.einsum('si,sj->ij', res_mask.astype(jnp.float32), full_mask.astype(jnp.float32))
    return update / (1e-3 + overlap)[:, :, None]


def tri_gates(pair_rows, mask_rows, w_proj):
    tri_dim = (w_proj.shape[1] - pair_rows.shape[-1]) // 4
    projected = dense(layer_norm(pair_rows), w_proj)
    mask_f = mask_rows.astype(jnp.float32)[:, :, None]
    left_act = (mask_f * jax.nn.sigmoid(projected[..., 2 * tri_dim:3 * tri_dim]) * projected[..., :tri_dim]).astype(jnp.bfloat16)
    right_act = (mask_f * jax.nn.sigmoid(projected[..., 3 * tri_dim:4 * tri_dim]) * projected[..., tri_dim:2 * tri_dim]).astype(jnp.bfloat16)
    gate_act = jax.nn.sigmoid(projected[..., 4 * tri_dim:])
    return left_act, right_act, gate_act


def tri_finish(product, gate_act, w_out):
    return gate_act * dense(layer_norm(product), w_out)


def pair_stack(pair_loc, pair_mask, pair_mask_t, pair_w):
    (tmo_proj, tmo_out, tmi_proj, tmi_out, tas_qkvg, tas_bias, tas_out,
     tae_qkvg, tae_bias, tae_out, ptr_in, ptr_out) = pair_w
    left_act, right_act, gate_act = tri_gates(pair_loc, pair_mask, tmo_proj)
    right_full = lax.all_gather(right_act, GROUP_AXIS, axis=0, tiled=True)
    product = jnp.einsum('ikc,jkc->ijc', left_act, right_full, preferred_element_type=jnp.float32)
    pair_loc = residual(pair_loc, tri_finish(product, gate_act, tmo_out))
    left_act, right_act, gate_act = tri_gates(pair_loc, pair_mask, tmi_proj)
    left_cols = lax.all_to_all(left_act, GROUP_AXIS, 1, 0, tiled=True)
    right_full = lax.all_gather(right_act, GROUP_AXIS, axis=0, tiled=True)
    product = jnp.einsum('kic,kjc->ijc', left_cols, right_full, preferred_element_type=jnp.float32)
    pair_loc = residual(pair_loc, tri_finish(product, gate_act, tmi_out))
    pair_loc = attention(pair_loc, pair_mask, tas_qkvg, tas_out, pair_bias_full(pair_loc, tas_bias))
    pair_cols = lax.all_to_all(pair_loc, GROUP_AXIS, 1, 0, tiled=True)
    pair_t = jnp.swapaxes(pair_cols, 0, 1)
    pair_t = attention(pair_t, pair_mask_t, tae_qkvg, tae_out, pair_bias_full(pair_t, tae_bias), (ptr_in, ptr_out))
    return jnp.swapaxes(lax.all_to_all(pair_t, GROUP_AXIS, 1, 0, tiled=True), 0, 1)


def evoformer_block(value_a7, pair_loc, full_mask, full_pair_mask, layer_w):
    (row_qkvg, row_bias, row_out, col_qkvg, col_out, mtr_in, mtr_out, opm_proj, opm_out) = layer_w[:9]
    shard_idx = lax.axis_index(GROUP_AXIS)
    seq_loc = value_a7.shape[0]
    res_loc = pair_loc.shape[0]
    seq_mask = lax.dynamic_slice_in_dim(full_mask, shard_idx * seq_loc, seq_loc, 0)
    res_mask = lax.dynamic_slice_in_dim(full_mask, shard_idx * res_loc, res_loc, 1)
    pair_mask = lax.dynamic_slice_in_dim(full_pair_mask, shard_idx * res_loc, res_loc, 0)
    pair_mask_t = lax.dynamic_slice_in_dim(full_pair_mask, shard_idx * res_loc, res_loc, 1).T
    value_a7 = attention(value_a7, seq_mask, row_qkvg, row_out, pair_bias_full(pair_loc, row_bias))
    array_b7 = jnp.swapaxes(lax.all_to_all(value_a7, GROUP_AXIS, 1, 0, tiled=True), 0, 1)
    array_b7 = attention(array_b7, res_mask.T, col_qkvg, col_out, None, (mtr_in, mtr_out))
    pair_loc = residual(pair_loc, outer_update(array_b7, res_mask, full_mask, opm_proj, opm_out))
    value_a7 = jnp.swapaxes(lax.all_to_all(array_b7, GROUP_AXIS, 1, 0, tiled=True), 0, 1)
    pair_loc = pair_stack(pair_loc, pair_mask, pair_mask_t, layer_w[9:])
    return value_a7, pair_loc


def solution(mesh):
    row_spec = P((PARTS_AXIS, GROUP_AXIS))

    def local_body(value_a7, pair_loc, value_a12, pair_mask_loc, *weights):
        full_mask = lax.all_gather(value_a12, GROUP_AXIS, axis=0, tiled=True)
        full_pair_mask = lax.all_gather(pair_mask_loc, GROUP_AXIS, axis=0, tiled=True)
        for layer_idx in range(weights[0].shape[0]):
            layer_w = tuple(weight[layer_idx] for weight in weights)
            value_a7, pair_loc = evoformer_block(value_a7, pair_loc, full_mask, full_pair_mask, layer_w)
        return value_a7, pair_loc

    def run_blocks(*arrays):
        n_weights = len(arrays) - 4
        return jax.shard_map(local_body, mesh=mesh, in_specs=(row_spec,) * 4 + (P(),) * n_weights, out_specs=(row_spec, row_spec), check_vma=False)(*arrays)

    return run_blocks
```
